128 devices in a mesh: grp: 16 (over y_hi, z, core), tp: 8 (over y_lo, x).
Axes of the slice: x: 4, y: 4 (y_hi: 2, y_lo: 2; y = y_hi * 2 + y_lo), z: 4, core: 2. Of those that a mesh axis runs over, the one named last changes fastest.
Arguments:
- tokens: bfloat16 [16384, 8192], P('grp'), may hold values from -12 to 12
- joined_weight: bfloat16 [8192, 10240], P(('grp', 'tp')), may hold values from -1.14904852 to 1.14904852
- rollout_lengths: int32 [128], P('grp'), may hold values from 1 to 128
- prompt_of: int32 [128, 1], P('grp'), may hold values from 0 to 15
- score_weight: bfloat16 [8192], P('tp'), may hold values from -0.52734375 to 0.52734375
Outputs:
- attention: bfloat16 [16384, 8192], P('grp', 'tp')
- advantages: float32 [128], P('grp')
The draws below stay inside these ranges and needn't reach their ends.
All inputs are finite; a program needn't handle non-finite values.
Results may differ from the reference program's by a relative error of at most 0.012.
The reference program's roundings to bfloat16 on the way count: a program that leaves them out, or rounds other values in their place, can miss the bound.
Values may be sent and summed in bfloat16 or wider, within the bound.
No kernel may reach another device: no remote copies, remote signals or barrier semaphores. Data moves between devices by JAX's collectives and lax.ppermute only.
A program may use at most 128 MiB of HBM per device.

```python
import jax
import jax.numpy as jnp
from jax import lax

MODEL_WIDTH = 8192
QUERY_HEADS = 64
KV_HEAD_COUNT = 8
HEAD_SIZE = 128
ROLL = 8
SLOT = 128
TOK_G = 1024
TOKENS = 16384
ROLLOUTS = 128
PROMPTS = 16
COLS = 10240
N_GRP = 16


def draw_tokens(key, part):
    values = jnp.clip(jax.random.normal(key, (TOKENS, MODEL_WIDTH), jnp.float32), -6.0, 6.0)
    return values.astype(jnp.bfloat16)


def draw_joined_weight(key, part):
    head_ratio = QUERY_HEADS // KV_HEAD_COUNT
    base_offset = jnp.clip(jax.random.normal(key, (MODEL_WIDTH, KV_HEAD_COUNT, head_ratio + 2, HEAD_SIZE), jnp.float32), -6.0, 6.0) * MODEL_WIDTH ** (-0.5)
    return base_offset.reshape(MODEL_WIDTH, COLS).astype(jnp.bfloat16)


def set_ends(entries, own_key, least, top_value):
    longest = entries.shape.index(max(entries.shape))
    spots = []
    for shift in (0, 1):
        where = [jax.random.randint(jax.random.fold_in(own_key, axis), (), 0, length) for axis, length in enumerate(entries.shape)]
        where[longest] = (where[longest] + shift) % entries.shape[longest]
        spots.append(tuple(where))
    return entries.at[spots[0]].set(least).at[spots[1]].set(top_value)


def levels(stream_key, extent, shards, low, high):
    level = 1.0
    for dim, parts in shards:
        steps = jax.random.uniform(jax.random.fold_in(jax.random.fold_in(stream_key, 6), dim), (parts,), jnp.float32, low / len(shards), high / len(shards))
        level = level * jnp.repeat(jnp.exp(steps), extent[dim] // parts).reshape((-1,) + (1,) * (len(extent) - 1 - dim))
    return level


def different_ones(rng, rows, amount, top, lift):
    sequence = jax.random.permutation(jax.random.fold_in(rng, 1), amount)
    boost = sequence
    for power in range(3):
        boost = boost * boost // amount
    boost = boost * lift // amount
    lots = jax.random.randint(jax.random.fold_in(rng, 2), (rows, amount), 0, 4096) + boost
    fixed_rows = jax.random.permutation(jax.random.fold_in(rng, 3), rows)[jnp.arange(amount) % rows]
    lots = jnp.where(jnp.arange(rows)[:, None] == fixed_rows[None, :], 1 << 14, lots)
    priority = lots * amount + jnp.arange(amount)
    return lax.top_k(priority.astype(jnp.int32), top)[1].astype(jnp.int32)


def normal_values(key, dims, deviation, limit, pieces=(), kind=jnp.bfloat16):
    factor_of = levels(key, dims, pieces, -0.22, 0.18) if pieces else 1.0
    result = jax.random.normal(key, dims, jnp.float32) * deviation * factor_of
    return jnp.minimum(jnp.maximum(result, -limit), limit).astype(kind)


def setup_inputs(seed: int = 0) -> dict:
    key_of = jax.random.split(jax.random.key(seed), 6)
    return {
        "tokens": draw_tokens(jax.random.fold_in(key_of[5], 71), 0),
        "joined_weight": draw_joined_weight(jax.random.fold_in(key_of[5], 71), 0),
        "rollout_lengths": set_ends(jax.random.randint(key_of[2], (ROLLOUTS,), 1, SLOT + 1), jax.random.fold_in(key_of[2], 1), 1, SLOT).astype(jnp.int32),
        "prompt_of": different_ones(key_of[3], ROLLOUTS, PROMPTS, 1, 0),
        "score_weight": normal_values(key_of[4], (QUERY_HEADS * HEAD_SIZE,), (8.0 / (QUERY_HEADS * HEAD_SIZE) ** 0.5), 0.52734375, ((0, 8),)),
    }


def attend(joined_matrix, rollout_length_list):
    head_ratio = QUERY_HEADS // KV_HEAD_COUNT
    slot_index = joined_matrix.shape[0] // rollout_length_list.shape[0]
    reshaped_tensor = joined_matrix.reshape(rollout_length_list.shape[0], slot_index, KV_HEAD_COUNT, head_ratio + 2, HEAD_SIZE).astype(jnp.float32)
    queries = reshaped_tensor[:, :, :, :head_ratio, :]
    key_heads = reshaped_tensor[:, :, :, head_ratio, :]
    value_heads = reshaped_tensor[:, :, :, head_ratio + 1, :]
    scores = jnp.einsum('rsgah,rtgh->rgast', queries, key_heads) * HEAD_SIZE ** (-0.5)
    positions = jnp.arange(slot_index)
    allowed = (positions[None, None, :] <= positions[None, :, None]) & (positions[None, None, :] < rollout_length_list[:, None, None])
    scores = jnp.where(allowed[:, None, None], scores, jnp.float32(-1e+30))
    peak = lax.optimization_barrier(jnp.max(scores, axis=-1, keepdims=True))
    expo = jnp.exp(scores - peak)
    probs = (expo / lax.optimization_barrier(jnp.sum(expo, axis=-1, keepdims=True))).astype(jnp.bfloat16)
    mixed = jnp.einsum('rgast,rtgh->rsgah', probs.astype(jnp.float32), value_heads)
    return mixed.reshape(joined_matrix.shape[0], QUERY_HEADS * HEAD_SIZE).astype(jnp.bfloat16)

def reference(tokens, joined_weight, rollout_lengths, prompt_of, score_weight):

    def one_group(items):
        group_tokens, rollout_length_list = items
        joined_matrix = jnp.dot(group_tokens, joined_weight, preferred_element_type=jnp.float32).astype(jnp.bfloat16)
        attention = attend(joined_matrix, rollout_length_list)
        token_score = jnp.dot(attention, score_weight, preferred_element_type=jnp.float32)
        valid = jnp.arange(SLOT)[None, :] < rollout_length_list[:, None]
        reward = lax.optimization_barrier(jnp.sum(jnp.where(valid, token_score.reshape(ROLL, SLOT), jnp.float32(0.0)), axis=1)) / rollout_length_list.astype(jnp.float32)
        return (attention, reward)
    attention, rewards = lax.map(one_group, (tokens.reshape(N_GRP, TOK_G, MODEL_WIDTH), rollout_lengths.reshape(N_GRP, ROLL)))
    attention = attention.reshape(TOKENS, QUERY_HEADS * HEAD_SIZE)
    rewards = rewards.reshape(ROLLOUTS)
    onehot = (prompt_of == jnp.arange(PROMPTS)[None, :]).astype(jnp.float32)
    counts = lax.optimization_barrier(jnp.sum(onehot, axis=0))
    totals = lax.optimization_barrier(jnp.sum(onehot * rewards[:, None], axis=0))
    squares = lax.optimization_barrier(jnp.sum(onehot * (rewards * rewards)[:, None], axis=0))
    divisor = jnp.maximum(counts, 1.0)
    average = totals / divisor
    spread = squares / divisor - average * average
    own_mean = lax.optimization_barrier(jnp.sum(onehot * average[None, :], axis=1))
    own_var = lax.optimization_barrier(jnp.sum(onehot * spread[None, :], axis=1))
    advantages = (rewards - own_mean) / jnp.sqrt(own_var + 0.25)
    return (attention, advantages)
```

```python
import functools

import jax
import jax.numpy as jnp
from jax import lax
from jax.experimental import pallas as pl
from jax.experimental.pallas import tpu as pltpu
from jax.sharding import PartitionSpec as P

HEAD = 128
RATIO = 8
Y_HI, Z, CORE = 2, 4, 2
Y_LO, X = 2, 4
AXES = ("grp", "tp")
EARLY = 4 * HEAD


def place(linear):
    g, t = divmod(linear, Y_LO * X)
    y_hi, rest = divmod(g, Z * CORE)
    z, core = divmod(rest, CORE)
    y_lo, x = divmod(t, X)
    return y_hi, y_lo, x, z, core


def index(y_hi, y_lo, x, z, core):
    return ((y_hi * Z + z % Z) * CORE + core) * (Y_LO * X) + y_lo * X + x


DEVICES = Y_HI * Y_LO * X * Z * CORE


def along_z(a, step):
    pairs = []
    for s in range(DEVICES):
        y_hi, y_lo, x, z, core = place(s)
        pairs.append((s, index(y_hi, y_lo, x, z + step, core)))
    return lax.ppermute(a, AXES, pairs)


def other_core(a):
    pairs = []
    for s in range(DEVICES):
        y_hi, y_lo, x, z, core = place(s)
        pairs.append((s, index(y_hi, y_lo, x, z, 1 - core)))
    return lax.ppermute(a, AXES, pairs)


def plane_groups():
    planes = {}
    for s in range(DEVICES):
        _, _, _, z, core = place(s)
        planes.setdefault((z, core), []).append(s)
    return list(planes.values())


def over_plane(a):
    return lax.all_to_all(a, AXES, 0, 0, tiled=True, axis_index_groups=plane_groups())


def product_kernel(counts, has_start, last, k_ref, tokens_ref, *refs):
    weights = refs[: len(counts)]
    start_ref = refs[len(counts)] if has_start else None
    out_ref, acc_ref = refs[-2:]
    step = pl.program_id(0)
    begin = 0
    for weight, count in zip(weights, counts):
        for first in (True, False):
            inside = (step == 0) if first else (step >= max(begin, 1)) & (step < begin + count)
            if first and begin > 0:
                continue

            @pl.when(inside)
            def _(weight=weight, first=first):
                block = weight[...].reshape(-1, weight.shape[-1])
                value = jnp.dot(tokens_ref[...], block, preferred_element_type=jnp.float32)
                if not first:
                    acc_ref[...] += value
                elif has_start:
                    acc_ref[...] = start_ref[...] + value
                else:
                    acc_ref[...] = value

        begin += count

    @pl.when(step == sum(counts) - 1)
    def _():
        out_ref[...] = acc_ref[...].astype(out_ref.dtype)


def product(tokens, pieces, start, last, name):
    counts = [len(ks) for _, ks in pieces]
    k_blocks = jnp.stack([k for _, ks in pieces for k in ks]).astype(jnp.int32)
    rows = tokens.shape[0]
    columns = pieces[0][0].shape[-1]
    total = sum(counts)
    in_specs = [pl.BlockSpec((rows, 512), lambda i, k: (0, k[i]))]
    begin = 0
    args = []
    for w, ks in pieces:
        n, depth = w.shape[0] // 8, w.shape[1]
        in_specs.append(
            pl.BlockSpec(
                (8, 1, 64, columns),
                functools.partial(
                    lambda i, k, b, n, d: (
                        jnp.clip(i - b, 0, n * d - 1) // d,
                        jnp.clip(i - b, 0, n * d - 1) % d,
                        0,
                        0,
                    ),
                    b=begin,
                    n=n,
                    d=depth,
                ),
            )
        )
        args.append(w)
        begin += len(ks)
    if start is not None:
        in_specs.append(pl.BlockSpec((rows, columns), lambda i, k: (0, 0)))
        args.append(start)
    return pl.pallas_call(
        functools.partial(product_kernel, counts, start is not None, last),
        out_shape=jax.ShapeDtypeStruct((rows, columns), jnp.bfloat16 if last else jnp.float32),
        grid_spec=pltpu.PrefetchScalarGridSpec(
            num_scalar_prefetch=1,
            grid=(total,),
            in_specs=in_specs,
            out_specs=pl.BlockSpec((rows, columns), lambda i, k: (0, 0)),
            scratch_shapes=[pltpu.VMEM((rows, columns), jnp.float32)],
        ),
        compiler_params=pltpu.CompilerParams(
            dimension_semantics=("arbitrary",), vmem_limit_bytes=40 * 1024 * 1024
        ),
        cost_estimate=pl.CostEstimate(
            flops=2 * rows * 512 * columns * total,
            bytes_accessed=total * 512 * (rows + columns) * 2 + rows * columns * 8,
            transcendentals=0,
        ),
        name=name,
    )(k_blocks, tokens, *args)


def attend_kernel(length_ref, early_ref, late_ref, w_ref, out_ref, reward_ref):
    r = pl.program_id(0)
    length = length_ref[r]
    key = late_ref[:, EARLY : EARLY + HEAD]
    value = late_ref[:, EARLY + HEAD :]
    slot = key.shape[0]
    row = lax.broadcasted_iota(jnp.int32, (slot, slot), 0)
    col = lax.broadcasted_iota(jnp.int32, (slot, slot), 1)
    allowed = (col <= row) & (col < length)
    live = (lax.broadcasted_iota(jnp.int32, (8, slot), 1) < length).astype(jnp.bfloat16)
    reward = jnp.zeros((8, HEAD), jnp.float32)
    for h in range(RATIO):
        src = early_ref if h < RATIO // 2 else late_ref
        at = (h % (RATIO // 2)) * HEAD
        q = src[:, at : at + HEAD]
        s = lax.dot_general(
            q, key, (((1,), (1,)), ((), ())), preferred_element_type=jnp.float32
        ) * (HEAD ** -0.5)
        s = jnp.where(allowed, s, jnp.float32(-1e30))
        e = jnp.exp(s - jnp.max(s, axis=-1, keepdims=True))
        p = (e / jnp.sum(e, axis=-1, keepdims=True)).astype(jnp.bfloat16)
        o = jnp.dot(p, value, preferred_element_type=jnp.float32).astype(jnp.bfloat16)
        out_ref[:, h * HEAD : (h + 1) * HEAD] = o
        total = jnp.dot(live, o, preferred_element_type=jnp.float32)
        reward += total * w_ref[:, h * HEAD : (h + 1) * HEAD]
    reward_ref[...] = jnp.sum(reward, axis=-1, keepdims=True)[None] / length.astype(
        jnp.float32
    ) * jnp.ones((1, 8, HEAD), jnp.float32)


def attend(early, late, lengths, score_weight):
    rows = early.shape[0]
    rolls = lengths.shape[0]
    slot = rows // rolls
    width = RATIO * HEAD
    out, reward = pl.pallas_call(
        attend_kernel,
        out_shape=(
            jax.ShapeDtypeStruct((rows, width), jnp.bfloat16),
            jax.ShapeDtypeStruct((rolls, 8, HEAD), jnp.float32),
        ),
        grid_spec=pltpu.PrefetchScalarGridSpec(
            num_scalar_prefetch=1,
            grid=(rolls,),
            in_specs=[
                pl.BlockSpec((slot, early.shape[1]), lambda r, n: (r, 0)),
                pl.BlockSpec((slot, late.shape[1]), lambda r, n: (r, 0)),
                pl.BlockSpec((1, width), lambda r, n: (0, 0)),
            ],
            out_specs=(
                pl.BlockSpec((slot, width), lambda r, n: (r, 0)),
                pl.BlockSpec((1, 8, HEAD), lambda r, n: (r, 0, 0)),
            ),
        ),
        compiler_params=pltpu.CompilerParams(dimension_semantics=("arbitrary",)),
        cost_estimate=pl.CostEstimate(
            flops=4 * rows * slot * width, bytes_accessed=rows * 2304 * 2, transcendentals=rows * slot * 8
        ),
        name="attend",
    )(lengths, early, late, score_weight.astype(jnp.float32).reshape(1, width))
    return out, reward[:, 0, 0]


def shards(tokens, joined_weight, rollout_lengths, prompt_of, score_weight):
    g = lax.axis_index("grp")
    z = (g // CORE) % Z
    core = g % CORE
    rows = joined_weight.shape[0]
    by_owner = joined_weight.reshape(rows, Y_LO * X, -1)

    def blocks(step, other, halves=(0, 1)):
        c = (1 - core) if other else core
        return [(h * Z + (z + step) % Z) * CORE + c for h in halves]

    def both_halves(a):
        return jnp.concatenate([a, a], axis=0)

    early = by_owner[:, :, :EARLY].transpose(1, 0, 2)
    late = by_owner[:, :, EARLY:].transpose(1, 0, 2)

    late_0 = over_plane(both_halves(late))[:, None]
    early_m = along_z(early, 1)
    early_p = along_z(early, -1)
    early_2a = along_z(early_m[: Y_LO * X // 2], 1)
    early_2b = along_z(early_p[Y_LO * X // 2 :], -1)

    early_first = over_plane(both_halves(jnp.stack([early, early_m, early_p], axis=1)))
    early_last = over_plane(both_halves(jnp.concatenate([early_2a, early_2b])[:, None]))

    late_m = along_z(late_0, 1)
    late_p = along_z(late_0, -1)
    late_2a = along_z(late_m[: Y_LO * X], 1)
    late_2b = along_z(late_p[Y_LO * X :], -1)

    late_acc = product(
        tokens,
        [(late_0, blocks(0, False)), (other_core(late_0), blocks(0, True))],
        None,
        False,
        "late0",
    )
    late_acc = product(
        tokens,
        [
            (late_m, blocks(-1, False)),
            (late_p, blocks(1, False)),
            (other_core(late_m), blocks(-1, True)),
            (other_core(late_p), blocks(1, True)),
        ],
        late_acc,
        False,
        "late1",
    )

    def three(other):
        a = [blocks(step, other) for step in (0, -1, 1)]
        return [a[s][h] for h in range(Y_HI) for s in range(3)]

    early_acc = product(
        tokens,
        [(early_first, three(False)), (other_core(early_first), three(True))],
        None,
        False,
        "early0",
    )
    late_done = product(
        tokens,
        [
            (late_2a, blocks(2, False, (0,))),
            (late_2b, blocks(2, False, (1,))),
            (other_core(late_2a), blocks(2, True, (0,))),
            (other_core(late_2b), blocks(2, True, (1,))),
        ],
        late_acc,
        True,
        "late2",
    )
    early_done = product(
        tokens,
        [(early_last, blocks(2, False)), (other_core(early_last), blocks(2, True))],
        early_acc,
        True,
        "early1",
    )
    attention, local_reward = attend(early_done, late_done, rollout_lengths, score_weight)

    mine = jnp.concatenate([local_reward, prompt_of[:, 0].astype(jnp.float32)])
    sent = jnp.broadcast_to(mine, (DEVICES, mine.shape[0]))
    got = lax.all_to_all(sent, AXES, 0, 0, tiled=True).reshape(-1, Y_LO * X, 2, mine.shape[0] // 2)
    rewards = jnp.sum(got[:, :, 0], axis=1)
    prompts = got[:, 0, 1]
    own_reward = lax.dynamic_index_in_dim(rewards, g, 0, keepdims=False)
    same = (prompts[None] == prompt_of.astype(jnp.float32)[:, :, None]).astype(jnp.float32)
    count = jnp.sum(same, axis=(1, 2))
    total = jnp.sum(same * rewards[None], axis=(1, 2))
    square = jnp.sum(same * (rewards * rewards)[None], axis=(1, 2))
    divisor = jnp.maximum(count, 1.0)
    mean = total / divisor
    var = square / divisor - mean * mean
    advantages = (own_reward - mean) / jnp.sqrt(var + 0.25)
    return (attention, advantages)


def solution(mesh):
    return jax.shard_map(
        shards,
        mesh=mesh,
        in_specs=(P("grp", None), P(("grp", "tp"), None), P("grp"), P("grp", None), P("tp")),
        out_specs=(P("grp", "tp"), P("grp")),
        check_vma=False,
    )
```
